256 devices in a mesh: row: 8 (over y, core), col: 32 (over z, x).
Axes of the slice: x: 4, y: 4, z: 8, core: 2. Of those that a mesh axis runs over, the one named last changes fastest.
Arguments:
- queries: bfloat16 [1024, 128, 1024], P(('row', 'col')), may hold values from -6 to 6
- coarse_keys: bfloat16 [2048, 1024], P('row'), may hold values from -6 to 6
- fine_keys: bfloat16 [16384, 1024], P('col'), may hold values from -6 to 6
- super_ids: int32 [1024, 16], P(('row', 'col')), may hold values from 0 to 2047, as said below
- picks: int32 [1024, 64], P(('row', 'col')), may hold values from 0 to 127, as said below
Outputs:
- importance: float32 [1024, 8, 2048], P(('row', 'col'))
- selected: float32 [1024, 512], P(('row', 'col'))
The draws below stay inside these ranges and needn't reach their ends.
Inputs may be any that keep to these rules, and one draw needn't show every extreme that they name: `super_ids`: within each aligned run of 4 query blocks (the query blocks of one device), at most 16 of the ids lie in any one aligned range of 64 superblocks, and some range holds exactly 16; in some aligned group of 32 consecutive runs, one range holds exactly 16 ids of every run. Ids may repeat. `picks`: the numbers of a row are distinct; pick p names fine block p % 8 of superblock super_ids[b, p // 8]. Within each aligned run of 4 query blocks, at most 64 of the named fine blocks lie in any one aligned range of 64 superblocks, and some range holds exactly 64.
All inputs are finite; a program needn't handle non-finite values.
Results may differ from the reference program's by a relative error of at most 0.0003.
Values may be sent and summed in bfloat16 or wider, within the bound.
A program may use at most 64 MiB of HBM per device.

```python
import math
import jax
import jax.numpy as jnp
from jax import lax

H = 8
D = 128
QTOK = 128
SBLK = 8
NSEL = 16
PICK = 64
SUP_DEV = 64
QB_DEV = 4
SUPERS = 2048
QB = 1024
N_ROW = 8
N_COL = 32


def summary_table(key, salt, count):
    inner = jax.random.fold_in(key, salt)
    values = jnp.clip(jax.random.normal(inner, (count, H * D), jnp.float32), -6.0, 6.0)
    return values.astype(jnp.bfloat16)


def draw_queries(key, part):
    inner = jax.random.fold_in(key, 11)
    values = jnp.clip(jax.random.normal(inner, (QB, QTOK, H * D), jnp.float32), -6.0, 6.0)
    return values.astype(jnp.bfloat16)


def draw_coarse_keys(key, part):
    return summary_table(key, 12, SUPERS)


def draw_fine_keys(key, part):
    return summary_table(key, 13, SUPERS * SBLK)


def draw_super_ids(key, part):
    devices_all = N_ROW * N_COL
    base_owner = jax.random.randint(jax.random.fold_in(key, 21), (N_ROW,), 0, N_COL)
    spread = jax.random.randint(jax.random.fold_in(key, 22), (N_ROW,), 1, N_COL)
    zero_row = jax.random.randint(jax.random.fold_in(key, 23), (), 0, N_ROW)
    spread = jnp.where(jnp.arange(N_ROW, dtype=jnp.int32) == zero_row, 0, spread)
    device_ids = jnp.arange(devices_all, dtype=jnp.int32)
    row_of = device_ids // N_COL
    col_of = device_ids % N_COL
    hot_owner = (base_owner[row_of] + col_of * spread[row_of]) % N_COL
    rotation = jax.random.randint(jax.random.fold_in(key, 24), (devices_all,), 0, 4)
    block_ids = jnp.arange(QB, dtype=jnp.int32)
    device_of = block_ids // QB_DEV
    quarter = block_ids % QB_DEV // (QB_DEV // 4)
    classes = (quarter + rotation[device_of]) % 4
    counts = jnp.where(classes > 0, (N_COL - 1 - classes) // 3 + 1, 1)
    member = jax.random.randint(jax.random.fold_in(key, 25), (QB, NSEL), 0, counts[:, None])
    offsets = jnp.where(classes[:, None] == 0, 0, classes[:, None] + 3 * member)
    owners = (hot_owner[device_of][:, None] + offsets) % N_COL
    local_ids = jax.random.randint(jax.random.fold_in(key, 26), (QB, NSEL), 0, SUP_DEV)
    return (owners * SUP_DEV + local_ids).astype(jnp.int32)


def draw_picks(key, part):
    candidates = NSEL * SBLK
    scores = jax.random.randint(jax.random.fold_in(key, 31), (QB, candidates), 0, 2 ** 20)
    scores = scores * candidates + jnp.arange(candidates, dtype=jnp.int32)[None, :]
    order = jnp.argsort(scores, axis=-1)
    return order[:, :PICK].astype(jnp.int32)


def setup_inputs(seed: int = 0) -> dict:
    streams_of = jax.random.split(jax.random.key(seed), 6)
    queries = draw_queries(jax.random.fold_in(streams_of[5], 71), 0)
    coarse_keys = draw_coarse_keys(jax.random.fold_in(streams_of[5], 71), 0)
    fine_keys = draw_fine_keys(jax.random.fold_in(streams_of[5], 71), 0)
    super_ids = draw_super_ids(jax.random.fold_in(streams_of[5], 71), 0)
    picks = draw_picks(jax.random.fold_in(streams_of[5], 71), 0)
    return dict(queries=queries, coarse_keys=coarse_keys, fine_keys=fine_keys, super_ids=super_ids, picks=picks)


def reference(queries, coarse_keys, fine_keys, super_ids, picks):
    factor = 1.0 / math.sqrt(D)
    qheads = queries.reshape(QB, QTOK, H, D)
    coarse_heads = coarse_keys.reshape(SUPERS, H, D).astype(jnp.float32)

    def coarse_block(query_block):
        scores = jnp.einsum('thd,chd->htc', query_block.astype(jnp.float32), coarse_heads) * factor
        softened = jax.nn.softmax(scores, axis=-1)
        return lax.optimization_barrier(jnp.sum(softened, axis=1)) * (SUPERS / QTOK)
    importance = lax.map(coarse_block, qheads)
    parents = jnp.take_along_axis(super_ids, (picks // SBLK).astype(jnp.int32), axis=1).astype(jnp.int32)
    fine_ids = (parents * SBLK + picks % SBLK).astype(jnp.int32)
    weights = jnp.take_along_axis(importance, jnp.broadcast_to(parents[:, None, :], (QB, H, PICK)), axis=2)

    def fine_block(inputs):
        query_block, block_ids, block_weights = inputs
        fetched = jnp.take(fine_keys, block_ids, axis=0).reshape(PICK, H, D).astype(jnp.float32)
        scores = jnp.einsum('thd,jhd->htj', query_block.astype(jnp.float32), fetched) * factor
        softened = jax.nn.softmax(scores, axis=-1)
        return (lax.optimization_barrier(jnp.sum(softened, axis=1)) * block_weights * (PICK / QTOK)).reshape(H * PICK)
    selected = lax.map(fine_block, (qheads, fine_ids, weights))
    return (importance, selected)
```

```python
import functools
import math

import jax
import jax.numpy as jnp
from jax import lax
from jax.experimental import pallas as pl
from jax.experimental.pallas import tpu as pltpu
from jax.sharding import PartitionSpec as P

H = 8
D = 128
SBLK = 8
PICK = 64
NSEL = 16
LOG2E = 1.4426950408889634

K, X, Y, Z = 2, 4, 4, 8
G = 2 * Y
SUB = 32
STEPS = 14


def kernel(
    q_ref, ck_ref, fk_ref, sid_ref, pk_ref,
    imp_ref, sel_ref,
    table, ck, qb, s_buf, idv, pkv, ids, res, irecv, fres, frecv,
    cs, cr, cds, cdr, qs, qr, ns, nr, ms, mr, xs, xr,
    rs, rr, ls, lr, ds, dr, os_, or_, fs, fr, loc,
):
    NB, T, _ = q_ref.shape
    S = Y * K * ck_ref.shape[0]
    CH = ck_ref.shape[0]
    factor = LOG2E / math.sqrt(D)
    row = lax.axis_index("row")
    col = lax.axis_index("col")
    y, k = row // K, row % K
    z, x = col // X, col % X
    par = x % 2
    me = 2 * y + par

    def at(yy, kk, zz, xx):
        return {"row": yy * K + kk, "col": zz * X + xx}

    def remote(src, dst, send, recv, dev):
        return pltpu.make_async_remote_copy(
            src_ref=src, dst_ref=dst, send_sem=send, recv_sem=recv,
            device_id=dev, device_id_type=pl.DeviceIdType.MESH,
        )

    def arrived(dst, sem):
        pltpu.make_async_copy(dst, dst, sem).wait()

    def peer(n):
        m = n // 2
        yy = (y + m + (m // 2) * (1 - 2 * (m % 2))) % Y
        pp = (par + n) % 2
        return 2 * yy + pp, at(yy, k, z, (x // 2) * 2 + pp)

    def heads(h):
        return pl.ds(pl.multiple_of(h * D, D), D)

    def piece(zz, xx, kk):
        return table.at[pl.ds((zz * X + xx) * (K * SUB) + kk * SUB, SUB)]

    def ck_slot(yy, kk):
        return ck.at[yy * K + kk]

    partner = at(y, 1 - k, z, x)
    right, left = at(y, k, (z + 1) % Z, x), at(y, k, (z + Z - 1) % Z, x)

    greet = [peer(n)[1] for n in range(1, G)]
    greet += [at(y, k, z, (x + 2) % X), at(y, k, z, (x + X - 1 + 2 * par) % X)]
    greet += [right, left, partner]
    barrier = pltpu.get_barrier_semaphore()
    for dev in greet:
        pl.semaphore_signal(barrier, inc=1, device_id=dev, device_id_type=pl.DeviceIdType.MESH)
    pl.semaphore_wait(barrier, len(greet))

    out = []
    for i in range(1, Y):
        yy = (y + i) % Y
        c = remote(ck_ref.at[:, heads(2 * yy + par)], ck_slot(y, k), cs.at[i - 1], cr.at[i - 1],
                   at(yy, k, z, x))
        c.start()
        out.append(c)
    own = fk_ref.at[pl.ds(k * SUB, SUB), :, heads(me)]
    mine = piece(z, x, k)
    remote(own, mine, rs, rr.at[0], right).start()
    remote(own, mine, ls, lr.at[0], left).start()
    for i in range(1, X):
        xx = (x + X - i) % X
        c = remote(fk_ref.at[pl.ds(k * SUB, SUB), :, heads(2 * y + xx % 2)], mine,
                   xs.at[i - 1], xr.at[i - 1], at(y, k, z, xx))
        c.start()
        out.append(c)
    c = remote(ck_ref.at[:, heads(me)], ck_slot(y, k), cds.at[0], cdr.at[0], partner)
    c.start()
    out.append(c)
    remote(own, mine, ds, dr, partner).start()
    local = [
        pltpu.make_async_copy(ck_ref.at[:, heads(me)], ck_slot(y, k), loc.at[0]),
        pltpu.make_async_copy(q_ref.at[:, :, heads(me)], qb.at[me], loc.at[1]),
        pltpu.make_async_copy(own, mine, loc.at[2]),
        pltpu.make_async_copy(sid_ref, idv.at[me], loc.at[3]),
        pltpu.make_async_copy(pk_ref, pkv.at[me], loc.at[4]),
    ]
    for c in local:
        c.start()
    for n in range(1, G):
        g, dev = peer(n)
        for c in (
            remote(q_ref.at[:, :, heads(g)], qb.at[me], qs.at[n - 1], qr.at[me], dev),
            remote(sid_ref, idv.at[me], ns.at[n - 1], nr.at[me], dev),
            remote(pk_ref, pkv.at[me], ms.at[n - 1], mr.at[me], dev),
        ):
            c.start()
            out.append(c)

    for s in range(1, X):
        p = piece(z, (x + s) % X, k)
        arrived(p, xr.at[s - 1])
        remote(p, p, rs, rr.at[s], right).start()
        remote(p, p, ls, lr.at[s], left).start()
        remote(p, p, ds, dr, partner).start()

    def ring(i):
        d = i // X + 1
        sub = i % X
        p = piece((z + Z - d) % Z, (x + sub) % X, k)
        arrived(p, rr.at[i])

        @pl.when(i < STEPS - X)
        def _():
            remote(p, p, rs, rr.at[i + X], right).start()

        remote(p, p, ds, dr, partner).start()
        o = piece((z + d) % Z, (x + sub + 2 * (i // (3 * X))) % X, k)
        arrived(o, lr.at[i])

        @pl.when(i < 2 * X)
        def _():
            remote(o, o, ls, lr.at[i + X], left).start()

        @pl.when((i >= STEPS - X) & (i < 3 * X))
        def _():
            remote(o, o, ls, lr.at[i + 2], left).start()

        remote(o, o, ds, dr, partner).start()

    def wait_queries(n):
        g, _ = peer(n)
        arrived(qb.at[g], qr.at[g])

    def dots(u):
        g, _ = peer(u // NB)
        qq = qb[g, u % NB]
        for r in range(Y * K):
            s_buf[u % 2, :, r * CH:(r + 1) * CH] = lax.dot_general(
                qq, ck[r], (((1,), (1,)), ((), ())), preferred_element_type=jnp.float32
            )

    def soften(u):
        g, _ = peer(u // NB)
        b = u % NB
        acc = jnp.zeros((8, S), jnp.float32)
        for t in range(T // 8):
            sc = s_buf[u % 2, t * 8:(t + 1) * 8, :]
            top = jnp.max(sc, axis=1, keepdims=True)
            e = jnp.exp2(sc * factor - top * factor)
            acc = acc + e * (1.0 / jnp.sum(e, axis=1, keepdims=True))
        total = jnp.sum(acc, axis=0, keepdims=True) * (S / T)
        for j in range(S // D):
            res[g, b, j:j + 1, :] = total[:, j * D:(j + 1) * D]

    def send_importance(n):
        g, dev = peer(n)
        return remote(res.at[g], irecv.at[me], os_.at[n], or_.at[me], dev)

    def block(u, carry):
        nxt = jnp.minimum(u + 1, G * NB - 1)

        @pl.when((u % NB == NB - 1) & (u < (G - 1) * NB))
        def _():
            wait_queries(nxt // NB)

        @pl.when((u % NB == 0) & (u >= 3 * NB))
        def _():
            send_importance(u // NB - 2).start()

        dots(nxt)
        soften(u)
        return carry

    ring(0)
    for i in range(1, Y):
        slot = ck_slot((y + Y - i) % Y, k)
        arrived(slot, cr.at[i - 1])
        c = remote(slot, slot, cds.at[i], cdr.at[i], partner)
        c.start()
        out.append(c)
    local[0].wait()
    for i in range(Y):
        arrived(ck_slot((y + Y - i) % Y, 1 - k), cdr.at[i])
    local[1].wait()
    dots(0)

    def tick(i, carry):
        ring(i)
        lax.fori_loop(jnp.minimum(3 * (i - 1), G * NB), jnp.minimum(3 * i, G * NB), block, 0)
        return carry

    lax.fori_loop(1, STEPS, tick, 0)
    for n in (G - 2, G - 1):
        send_importance(n).start()

    for n in range(1, G):
        g, _ = peer(n)
        arrived(idv.at[g], nr.at[g])
        arrived(pkv.at[g], mr.at[g])
    for c in local[2:]:
        c.wait()
    to_smem = pltpu.make_async_copy(idv, ids, loc.at[5])
    to_smem.start()
    to_smem.wait()
    half = table.at[pl.ds(0, table.shape[0] // 2)]
    arrived(half, dr)

    def send_picked(n):
        g, dev = peer(n)
        return remote(fres.at[g], frecv.at[me], fs.at[n], fr.at[me], dev)

    place = lax.broadcasted_iota(jnp.int32, (NSEL * SBLK, PICK), 0)

    def fine(n):
        g, _ = peer(n)
        for b in range(NB):
            rows = [table[ids[g, b, s]].astype(jnp.float32) for s in range(NSEL)]
            cand = jnp.concatenate(rows, axis=0).astype(jnp.bfloat16)
            sc = lax.dot_general(
                cand, qb[g, b], (((1,), (1,)), ((), ())), preferred_element_type=jnp.float32
            )
            hit = (place == pkv[g, b:b + 1, :]).astype(jnp.float32)
            picked = jnp.max(hit, axis=1, keepdims=True) > 0.0
            sc = jnp.where(picked, sc * factor, -1e30)
            top = jnp.max(sc, axis=0, keepdims=True)
            e = jnp.exp2(sc - top)
            e = e * (1.0 / jnp.sum(e, axis=0, keepdims=True))
            val = jnp.sum(e, axis=1, keepdims=True)
            fres[g, b:b + 1, :] = jnp.sum(hit * val, axis=0, keepdims=True)

    def fine_step(n, carry):
        @pl.when(n > 1)
        def _():
            send_picked(n - 1).start()

        fine(n)
        return carry

    lax.fori_loop(1, G, fine_step, 0)
    fine(0)
    send_picked(G - 1).start()
    frecv[me] = fres[me]
    irecv[me] = res[me]

    for n in range(1, G):
        g, _ = peer(n)
        arrived(irecv.at[g], or_.at[g])
    for b in range(NB):
        for j in range(S // D):
            imp_ref[b, j] = irecv[:, b, j, :]
    lane = lax.broadcasted_iota(jnp.int32, (H, D), 1)
    weights = []
    for b in range(NB):
        owner = lax.shift_right_logical(pkv[me, b:b + 1, :], 3)
        w = jnp.zeros((H, PICK), jnp.float32)
        for s in range(NSEL):
            sid = ids[me, b, s]
            part = imp_ref[b, lax.shift_right_logical(sid, 7)]
            one = jnp.sum(jnp.where(lane == (sid & (D - 1)), part, 0.0), axis=1, keepdims=True)
            w = w + jnp.where(owner == s, one, 0.0)
        weights.append(w * (PICK / T))
    for n in range(1, G):
        g, _ = peer(n)
        arrived(frecv.at[g], fr.at[g])
    for b in range(NB):
        sel_ref[b] = frecv[:, b, :] * weights[b]

    for c in out:
        c.wait_send()
    for n in range(1, G):
        send_importance(n).wait_send()
        send_picked(n).wait_send()
    arrived(table.at[pl.ds(0, STEPS * SUB)], rs)
    arrived(table.at[pl.ds(0, STEPS * SUB)], ls)
    arrived(half, ds)


def per_device(queries, coarse_keys, fine_keys, super_ids, picks):
    nb, t, width = queries.shape
    ch = coarse_keys.shape[0]
    s = ch * Y * K
    dma = pltpu.SemaphoreType.DMA
    f32, bf16, i32 = jnp.float32, jnp.bfloat16, jnp.int32
    imp, sel = pl.pallas_call(
        kernel,
        out_shape=(
            jax.ShapeDtypeStruct((nb, s // D, H, D), f32),
            jax.ShapeDtypeStruct((nb, H, PICK), f32),
        ),
        in_specs=[pl.BlockSpec(memory_space=pl.ANY)] * 5,
        out_specs=[pl.BlockSpec(memory_space=pltpu.VMEM)] * 2,
        scratch_shapes=[
            pltpu.VMEM((s, SBLK, D), bf16),
            pltpu.VMEM((Y * K, ch, D), bf16),
            pltpu.VMEM((G, nb, t, D), bf16),
            pltpu.VMEM((2, t, s), f32),
            pltpu.VMEM((G, nb, NSEL), i32),
            pltpu.VMEM((G, nb, PICK), i32),
            pltpu.SMEM((G, nb, NSEL), i32),
            pltpu.VMEM((G, nb, s // D, D), f32),
            pltpu.VMEM((G, nb, s // D, D), f32),
            pltpu.VMEM((G, nb, PICK), f32),
            pltpu.VMEM((G, nb, PICK), f32),
            dma((Y - 1,)), dma((Y - 1,)), dma((Y,)), dma((Y,)),
            dma((G - 1,)), dma((G,)), dma((G - 1,)), dma((G,)), dma((G - 1,)), dma((G,)),
            dma((X - 1,)), dma((X - 1,)),
            dma, dma((STEPS,)), dma, dma((STEPS,)), dma, dma,
            dma((G,)), dma((G,)), dma((G,)), dma((G,)), dma((6,)),
        ],
        compiler_params=pltpu.CompilerParams(collective_id=0, has_side_effects=True),
    )(queries, coarse_keys, fine_keys.reshape(-1, SBLK, width), super_ids, picks)
    return imp.transpose(0, 2, 1, 3).reshape(nb, H, s), sel.reshape(nb, H * PICK)


def solution(mesh):
    return jax.shard_map(
        per_device,
        mesh=mesh,
        in_specs=(
            P(("row", "col"), None, None),
            P("row", None),
            P("col", None),
            P(("row", "col"), None),
            P(("row", "col"), None),
        ),
        out_specs=(P(("row", "col"), None, None), P(("row", "col"), None)),
        check_vma=False,
    )
```

```python
import functools
import math

import jax
import jax.numpy as jnp
from jax import lax
from jax.experimental import pallas as pl
from jax.experimental.pallas import tpu as pltpu
from jax.sharding import PartitionSpec as P

H = 8
D = 128
SBLK = 8
PICK = 64
NSEL = 16
LOG2E = 1.4426950408889634

K, X, Y, Z = 2, 4, 4, 8
G = 2 * Y
SUB = 32
STEPS = 14


def kernel(
    q_ref, ck_ref, fk_ref, sid_ref, pk_ref,
    imp_ref, sel_ref,
    table, ck, qb, s_even, s_odd, e_buf, idv, pkv, ids, res, irecv, fres, frecv,
    cs, cr, cds, cdr, qs, qr, ns, nr, ms, mr, xs, xr,
    rs, rr, ls, lr, ds, dr, os_, or_, fs, fr, loc,
):
    NB, T, _ = q_ref.shape
    S = Y * K * ck_ref.shape[0]
    CH = ck_ref.shape[0]
    PER = Y * K // NB
    factor = LOG2E / math.sqrt(D)
    row = lax.axis_index("row")
    col = lax.axis_index("col")
    y, k = row // K, row % K
    z, x = col // X, col % X
    par = x % 2
    me = 2 * y + par

    def at(yy, kk, zz, xx):
        return {"row": yy * K + kk, "col": zz * X + xx}

    def remote(src, dst, send, recv, dev):
        return pltpu.make_async_remote_copy(
            src_ref=src, dst_ref=dst, send_sem=send, recv_sem=recv,
            device_id=dev, device_id_type=pl.DeviceIdType.MESH,
        )

    def arrived(dst, sem):
        pltpu.make_async_copy(dst, dst, sem).wait()

    def peer(n):
        m = n // 2
        yy = (y + m + (m // 2) * (1 - 2 * (m % 2))) % Y
        pp = (par + n) % 2
        return 2 * yy + pp, at(yy, k, z, (x // 2) * 2 + pp)

    def heads(h):
        return pl.ds(pl.multiple_of(h * D, D), D)

    def piece(zz, xx, kk):
        return table.at[pl.ds((zz * X + xx) * (K * SUB) + kk * SUB, SUB)]

    def ck_slot(yy, kk):
        return ck.at[yy * K + kk]

    partner = at(y, 1 - k, z, x)
    right, left = at(y, k, (z + 1) % Z, x), at(y, k, (z + Z - 1) % Z, x)

    greet = [peer(n)[1] for n in range(1, G)]
    greet += [at(y, k, z, (x + 2) % X), at(y, k, z, (x + X - 1 + 2 * par) % X)]
    greet += [right, left, partner]
    barrier = pltpu.get_barrier_semaphore()
    for dev in greet:
        pl.semaphore_signal(barrier, inc=1, device_id=dev, device_id_type=pl.DeviceIdType.MESH)
    pl.semaphore_wait(barrier, len(greet))

    out = []
    for i in range(1, Y):
        yy = (y + i) % Y
        c = remote(ck_ref.at[:, heads(2 * yy + par)], ck_slot(y, k), cs.at[i - 1], cr.at[i - 1],
                   at(yy, k, z, x))
        c.start()
        out.append(c)
    own = fk_ref.at[pl.ds(k * SUB, SUB), :, heads(me)]
    mine = piece(z, x, k)
    remote(own, mine, rs, rr.at[0], right).start()
    remote(own, mine, ls, lr.at[0], left).start()
    for i in range(1, X):
        xx = (x + X - i) % X
        c = remote(fk_ref.at[pl.ds(k * SUB, SUB), :, heads(2 * y + xx % 2)], mine,
                   xs.at[i - 1], xr.at[i - 1], at(y, k, z, xx))
        c.start()
        out.append(c)
    c = remote(ck_ref.at[:, heads(me)], ck_slot(y, k), cds.at[0], cdr.at[0], partner)
    c.start()
    out.append(c)
    remote(own, mine, ds, dr, partner).start()
    local = [
        pltpu.make_async_copy(ck_ref.at[:, heads(me)], ck_slot(y, k), loc.at[0]),
        pltpu.make_async_copy(q_ref.at[:, :, heads(me)], qb.at[me], loc.at[1]),
        pltpu.make_async_copy(own, mine, loc.at[2]),
        pltpu.make_async_copy(sid_ref, idv.at[me], loc.at[3]),
        pltpu.make_async_copy(pk_ref, pkv.at[me], loc.at[4]),
    ]
    for c in local:
        c.start()
    for n in range(1, G):
        g, dev = peer(n)
        for c in (
            remote(q_ref.at[:, :, heads(g)], qb.at[me], qs.at[n - 1], qr.at[me], dev),
            remote(sid_ref, idv.at[me], ns.at[n - 1], nr.at[me], dev),
            remote(pk_ref, pkv.at[me], ms.at[n - 1], mr.at[me], dev),
        ):
            c.start()
            out.append(c)

    for s in range(1, X):
        p = piece(z, (x + s) % X, k)
        arrived(p, xr.at[s - 1])
        remote(p, p, rs, rr.at[s], right).start()
        remote(p, p, ls, lr.at[s], left).start()
        remote(p, p, ds, dr, partner).start()

    def ring(i):
        d = i // X + 1
        sub = i % X
        p = piece((z + Z - d) % Z, (x + sub) % X, k)
        arrived(p, rr.at[i])

        @pl.when(i < STEPS - X)
        def _():
            remote(p, p, rs, rr.at[i + X], right).start()

        remote(p, p, ds, dr, partner).start()
        o = piece((z + d) % Z, (x + sub + 2 * (i // (3 * X))) % X, k)
        arrived(o, lr.at[i])

        @pl.when(i < 2 * X)
        def _():
            remote(o, o, ls, lr.at[i + X], left).start()

        @pl.when((i >= STEPS - X) & (i < 3 * X))
        def _():
            remote(o, o, ls, lr.at[i + 2], left).start()

        remote(o, o, ds, dr, partner).start()

    def wait_queries(n):
        g, _ = peer(n)
        arrived(qb.at[g], qr.at[g])

    def dots(n, s_buf, c):
        g, _ = peer(n)
        qq = qb[g].reshape(NB * T, D)
        for r in range(PER):
            sc = lax.dot_general(
                qq, ck[c * PER + r], (((1,), (1,)), ((), ())), preferred_element_type=jnp.float32
            )
            for j in range(CH // D):
                s_buf[(c * PER + r) * (CH // D) + j] = sc[:, j * D:(j + 1) * D]

    def soften(n, s_buf, b):
        g, _ = peer(n)
        rows = pl.ds(pl.multiple_of(b * T, T), T)
        top = s_buf[0, rows, :]
        for j in range(1, S // D):
            top = jnp.maximum(top, s_buf[j, rows, :])
        top = jnp.max(top, axis=1, keepdims=True) * factor
        z = None
        for j in range(S // D):
            e = jnp.exp2(s_buf[j, rows, :] * factor - top)
            e_buf[j] = e
            z = e if z is None else z + e
        w = (S / T) / jnp.sum(z, axis=1, keepdims=True)
        for j in range(S // D):
            res[g, b, j:j + 1, :] = jnp.sum(e_buf[j] * w, axis=0, keepdims=True)

    def send_importance(n):
        g, dev = peer(n)
        return remote(res.at[g], irecv.at[me], os_.at[n], or_.at[me], dev)

    def block(u, carry):
        n, b = u // NB, u % NB
        nxt = jnp.minimum(n + 1, G - 1)

        @pl.when((b == 0) & (n < G - 1))
        def _():
            wait_queries(nxt)

        @pl.when((b == 0) & (n >= 3))
        def _():
            send_importance(n - 2).start()

        @pl.when(n % 2 == 0)
        def _():
            dots(nxt, s_odd, b)
            soften(n, s_even, b)

        @pl.when(n % 2 == 1)
        def _():
            dots(nxt, s_even, b)
            soften(n, s_odd, b)

        return carry

    ring(0)
    for i in range(1, Y):
        slot = ck_slot((y + Y - i) % Y, k)
        arrived(slot, cr.at[i - 1])
        c = remote(slot, slot, cds.at[i], cdr.at[i], partner)
        c.start()
        out.append(c)
    local[0].wait()
    for i in range(Y):
        arrived(ck_slot((y + Y - i) % Y, 1 - k), cdr.at[i])
    local[1].wait()

    def first(c, carry):
        dots(0, s_even, c)
        return carry

    lax.fori_loop(0, NB, first, 0)

    def tick(i, carry):
        ring(i)
        lax.fori_loop(jnp.minimum(3 * (i - 1), G * NB), jnp.minimum(3 * i, G * NB), block, 0)
        return carry

    lax.fori_loop(1, STEPS, tick, 0)
    for n in (G - 2, G - 1):
        send_importance(n).start()

    for n in range(1, G):
        g, _ = peer(n)
        arrived(idv.at[g], nr.at[g])
        arrived(pkv.at[g], mr.at[g])
    for c in local[2:]:
        c.wait()
    to_smem = pltpu.make_async_copy(idv, ids, loc.at[5])
    to_smem.start()
    to_smem.wait()
    half = table.at[pl.ds(0, table.shape[0] // 2)]
    arrived(half, dr)

    def send_picked(n):
        g, dev = peer(n)
        return remote(fres.at[g], frecv.at[me], fs.at[n], fr.at[me], dev)

    place = lax.broadcasted_iota(jnp.int32, (NSEL * SBLK, PICK), 0)

    def fine(n):
        g, _ = peer(n)
        for b in range(NB):
            rows = [table[ids[g, b, s]].astype(jnp.float32) for s in range(NSEL)]
            cand = jnp.concatenate(rows, axis=0).astype(jnp.bfloat16)
            sc = lax.dot_general(
                cand, qb[g, b], (((1,), (1,)), ((), ())), preferred_element_type=jnp.float32
            )
            hit = (place == pkv[g, b:b + 1, :]).astype(jnp.float32)
            picked = jnp.max(hit, axis=1, keepdims=True) > 0.0
            sc = jnp.where(picked, sc * factor, -1e30)
            top = jnp.max(sc, axis=0, keepdims=True)
            e = jnp.exp2(sc - top)
            e = e * (1.0 / jnp.sum(e, axis=0, keepdims=True))
            val = jnp.sum(e, axis=1, keepdims=True)
            fres[g, b:b + 1, :] = jnp.sum(hit * val, axis=0, keepdims=True)

    def fine_step(n, carry):
        @pl.when(n > 1)
        def _():
            send_picked(n - 1).start()

        fine(n)
        return carry

    lax.fori_loop(1, G, fine_step, 0)
    fine(0)
    send_picked(G - 1).start()
    frecv[me] = fres[me]
    irecv[me] = res[me]

    for n in range(1, G):
        g, _ = peer(n)
        arrived(irecv.at[g], or_.at[g])
    for b in range(NB):
        for j in range(S // D):
            imp_ref[b, j] = irecv[:, b, j, :]
    lane = lax.broadcasted_iota(jnp.int32, (H, D), 1)
    weights = []
    for b in range(NB):
        owner = lax.shift_right_logical(pkv[me, b:b + 1, :], 3)
        w = jnp.zeros((H, PICK), jnp.float32)
        for s in range(NSEL):
            sid = ids[me, b, s]
            part = imp_ref[b, lax.shift_right_logical(sid, 7)]
            one = jnp.sum(jnp.where(lane == (sid & (D - 1)), part, 0.0), axis=1, keepdims=True)
            w = w + jnp.where(owner == s, one, 0.0)
        weights.append(w * (PICK / T))
    for n in range(1, G):
        g, _ = peer(n)
        arrived(frecv.at[g], fr.at[g])
    for b in range(NB):
        sel_ref[b] = frecv[:, b, :] * weights[b]

    for c in out:
        c.wait_send()
    for n in range(1, G):
        send_importance(n).wait_send()
        send_picked(n).wait_send()
    arrived(table.at[pl.ds(0, STEPS * SUB)], rs)
    arrived(table.at[pl.ds(0, STEPS * SUB)], ls)
    arrived(half, ds)


def per_device(queries, coarse_keys, fine_keys, super_ids, picks):
    nb, t, width = queries.shape
    ch = coarse_keys.shape[0]
    s = ch * Y * K
    dma = pltpu.SemaphoreType.DMA
    f32, bf16, i32 = jnp.float32, jnp.bfloat16, jnp.int32
    imp, sel = pl.pallas_call(
        kernel,
        out_shape=(
            jax.ShapeDtypeStruct((nb, s // D, H, D), f32),
            jax.ShapeDtypeStruct((nb, H, PICK), f32),
        ),
        in_specs=[pl.BlockSpec(memory_space=pl.ANY)] * 5,
        out_specs=[pl.BlockSpec(memory_space=pltpu.VMEM)] * 2,
        scratch_shapes=[
            pltpu.VMEM((s, SBLK, D), bf16),
            pltpu.VMEM((Y * K, ch, D), bf16),
            pltpu.VMEM((G, nb, t, D), bf16),
            pltpu.VMEM((s // D, nb * t, D), f32),
            pltpu.VMEM((s // D, nb * t, D), f32),
            pltpu.VMEM((s // D, t, D), f32),
            pltpu.VMEM((G, nb, NSEL), i32),
            pltpu.VMEM((G, nb, PICK), i32),
            pltpu.SMEM((G, nb, NSEL), i32),
            pltpu.VMEM((G, nb, s // D, D), f32),
            pltpu.VMEM((G, nb, s // D, D), f32),
            pltpu.VMEM((G, nb, PICK), f32),
            pltpu.VMEM((G, nb, PICK), f32),
            dma((Y - 1,)), dma((Y - 1,)), dma((Y,)), dma((Y,)),
            dma((G - 1,)), dma((G,)), dma((G - 1,)), dma((G,)), dma((G - 1,)), dma((G,)),
            dma((X - 1,)), dma((X - 1,)),
            dma, dma((STEPS,)), dma, dma((STEPS,)), dma, dma,
            dma((G,)), dma((G,)), dma((G,)), dma((G,)), dma((6,)),
        ],
        compiler_params=pltpu.CompilerParams(collective_id=0, has_side_effects=True),
    )(queries, coarse_keys, fine_keys.reshape(-1, SBLK, width), super_ids, picks)
    return imp.transpose(0, 2, 1, 3).reshape(nb, H, s), sel.reshape(nb, H * PICK)


def solution(mesh):
    return jax.shard_map(
        per_device,
        mesh=mesh,
        in_specs=(
            P(("row", "col"), None, None),
            P("row", None),
            P("col", None),
            P(("row", "col"), None),
            P(("row", "col"), None),
        ),
        out_specs=(P(("row", "col"), None, None), P(("row", "col"), None)),
        check_vma=False,
    )
```

```python
import functools
import math

import jax
import jax.numpy as jnp
from jax import lax
from jax.experimental import pallas as pl
from jax.experimental.pallas import tpu as pltpu
from jax.sharding import PartitionSpec as P

H = 8
D = 128
SBLK = 8
PICK = 64
NSEL = 16
LOG2E = 1.4426950408889634

K, X, Y, Z = 2, 4, 4, 8
G = 2 * Y
SUB = 32
STEPS = 14


def kernel(
    q_ref, ck_ref, fk_ref, sid_ref, pk_ref,
    imp_ref, sel_ref,
    table, ck, qb, s_even, s_odd, e_buf, idv, pkv, ids, res, irecv, fres, frecv, bias,
    cs, cr, cds, cdr, qs, qr, ns, nr, ms, mr, xs, xr,
    rs, rr, ls, lr, ds, dr, os_, or_, fs, fr, loc,
):
    NB, T, _ = q_ref.shape
    S = Y * K * ck_ref.shape[0]
    CH = ck_ref.shape[0]
    PER = Y * K // NB
    factor = LOG2E / math.sqrt(D)
    row = lax.axis_index("row")
    col = lax.axis_index("col")
    y, k = row // K, row % K
    z, x = col // X, col % X
    par = x % 2
    me = 2 * y + par

    def at(yy, kk, zz, xx):
        return {"row": yy * K + kk, "col": zz * X + xx}

    def remote(src, dst, send, recv, dev):
        return pltpu.make_async_remote_copy(
            src_ref=src, dst_ref=dst, send_sem=send, recv_sem=recv,
            device_id=dev, device_id_type=pl.DeviceIdType.MESH,
        )

    def arrived(dst, sem):
        pltpu.make_async_copy(dst, dst, sem).wait()

    def peer(n):
        m = n // 2
        yy = (y + m + (m // 2) * (1 - 2 * (m % 2))) % Y
        pp = (par + n) % 2
        return 2 * yy + pp, at(yy, k, z, (x // 2) * 2 + pp)

    def heads(h):
        return pl.ds(pl.multiple_of(h * D, D), D)

    def piece(zz, xx, kk):
        return table.at[pl.ds((zz * X + xx) * (K * SUB) + kk * SUB, SUB)]

    def ck_slot(yy, kk):
        return ck.at[yy * K + kk]

    partner = at(y, 1 - k, z, x)
    right, left = at(y, k, (z + 1) % Z, x), at(y, k, (z + Z - 1) % Z, x)

    greet = [peer(n)[1] for n in range(1, G)]
    greet += [at(y, k, z, (x + 2) % X), at(y, k, z, (x + X - 1 + 2 * par) % X)]
    greet += [right, left, partner]
    barrier = pltpu.get_barrier_semaphore()
    for dev in greet:
        pl.semaphore_signal(barrier, inc=1, device_id=dev, device_id_type=pl.DeviceIdType.MESH)
    pl.semaphore_wait(barrier, len(greet))

    out = []
    for i in range(1, Y):
        yy = (y + i) % Y
        c = remote(ck_ref.at[:, heads(2 * yy + par)], ck_slot(y, k), cs.at[i - 1], cr.at[i - 1],
                   at(yy, k, z, x))
        c.start()
        out.append(c)
    own = fk_ref.at[pl.ds(k * SUB, SUB), :, heads(me)]
    mine = piece(z, x, k)
    remote(own, mine, rs, rr.at[0], right).start()
    remote(own, mine, ls, lr.at[0], left).start()
    for i in range(1, X):
        xx = (x + X - i) % X
        c = remote(fk_ref.at[pl.ds(k * SUB, SUB), :, heads(2 * y + xx % 2)], mine,
                   xs.at[i - 1], xr.at[i - 1], at(y, k, z, xx))
        c.start()
        out.append(c)
    c = remote(ck_ref.at[:, heads(me)], ck_slot(y, k), cds.at[0], cdr.at[0], partner)
    c.start()
    out.append(c)
    remote(own, mine, ds, dr, partner).start()
    local = [
        pltpu.make_async_copy(ck_ref.at[:, heads(me)], ck_slot(y, k), loc.at[0]),
        pltpu.make_async_copy(q_ref.at[:, :, heads(me)], qb.at[me], loc.at[1]),
        pltpu.make_async_copy(own, mine, loc.at[2]),
        pltpu.make_async_copy(sid_ref, idv.at[me], loc.at[3]),
        pltpu.make_async_copy(pk_ref, pkv.at[me], loc.at[4]),
    ]
    for c in local:
        c.start()
    for n in range(1, G):
        g, dev = peer(n)
        for c in (
            remote(sid_ref, idv.at[me], ns.at[n - 1], nr.at[me], dev),
            remote(pk_ref, pkv.at[me], ms.at[n - 1], mr.at[me], dev),
        ):
            c.start()
            out.append(c)
    for n in range(1, G):
        g, dev = peer(n)
        c = remote(q_ref.at[:, :, heads(g)], qb.at[me], qs.at[n - 1], qr.at[me], dev)
        c.start()
        out.append(c)

    for s in range(1, X):
        p = piece(z, (x + s) % X, k)
        arrived(p, xr.at[s - 1])
        remote(p, p, rs, rr.at[s], right).start()
        remote(p, p, ls, lr.at[s], left).start()
        remote(p, p, ds, dr, partner).start()

    def ring(i):
        d = i // X + 1
        sub = i % X
        p = piece((z + Z - d) % Z, (x + sub) % X, k)
        arrived(p, rr.at[i])

        @pl.when(i < STEPS - X)
        def _():
            remote(p, p, rs, rr.at[i + X], right).start()

        remote(p, p, ds, dr, partner).start()
        o = piece((z + d) % Z, (x + sub + 2 * (i // (3 * X))) % X, k)
        arrived(o, lr.at[i])

        @pl.when(i < 2 * X)
        def _():
            remote(o, o, ls, lr.at[i + X], left).start()

        @pl.when((i >= STEPS - X) & (i < 3 * X))
        def _():
            remote(o, o, ls, lr.at[i + 2], left).start()

        remote(o, o, ds, dr, partner).start()

    def wait_queries(n):
        g, _ = peer(n)
        arrived(qb.at[g], qr.at[g])

    def dots(n, s_buf, c):
        g, _ = peer(n)
        qq = qb[g].reshape(NB * T, D)
        for r in range(PER):
            sc = lax.dot_general(
                qq, ck[c * PER + r], (((1,), (1,)), ((), ())), preferred_element_type=jnp.float32
            )
            for j in range(CH // D):
                s_buf[(c * PER + r) * (CH // D) + j] = sc[:, j * D:(j + 1) * D]

    def soften(n, s_buf, b):
        g, _ = peer(n)
        rows = pl.ds(pl.multiple_of(b * T, T), T)
        top = s_buf[0, rows, :]
        for j in range(1, S // D):
            top = jnp.maximum(top, s_buf[j, rows, :])
        top = jnp.max(top, axis=1, keepdims=True) * factor
        z = None
        for j in range(S // D):
            e = jnp.exp2(s_buf[j, rows, :] * factor - top)
            e_buf[j] = e
            z = e if z is None else z + e
        w = (S / T) / jnp.sum(z, axis=1, keepdims=True)
        for j in range(S // D):
            res[g, b, j:j + 1, :] = jnp.sum(e_buf[j] * w, axis=0, keepdims=True)

    def send_importance(n):
        g, dev = peer(n)
        return remote(res.at[g], irecv.at[me], os_.at[n], or_.at[me], dev)

    def block(u, carry):
        n, b = u // NB, u % NB
        nxt = jnp.minimum(n + 1, G - 1)

        @pl.when((b == 0) & (n < G - 1))
        def _():
            wait_queries(nxt)

        @pl.when((b == 0) & (n >= 3))
        def _():
            send_importance(n - 2).start()

        @pl.when(n % 2 == 0)
        def _():
            dots(nxt, s_odd, b)
            soften(n, s_even, b)

        @pl.when(n % 2 == 1)
        def _():
            dots(nxt, s_even, b)
            soften(n, s_odd, b)

        return carry

    ring(0)
    for i in range(1, Y):
        slot = ck_slot((y + Y - i) % Y, k)
        arrived(slot, cr.at[i - 1])
        c = remote(slot, slot, cds.at[i], cdr.at[i], partner)
        c.start()
        out.append(c)
    place = lax.broadcasted_iota(jnp.int32, (NSEL * SBLK, 2 * PICK), 0)
    mine_half = lax.broadcasted_iota(jnp.int32, (1, 2 * PICK), 1) // PICK == par

    def hits(g, b):
        row = jnp.concatenate([pkv[g, b:b + 1, :]] * 2, axis=1)
        return place == jnp.where(mine_half, row, -1)

    def masks():
        for n in range(1, G):
            g, _ = peer(n)
            arrived(idv.at[g], nr.at[g])
            arrived(pkv.at[g], mr.at[g])
        for c in local[2:]:
            c.wait()
        to_smem = pltpu.make_async_copy(idv, ids, loc.at[5])
        to_smem.start()

        def one(g, carry):
            for b in range(NB):
                found = jnp.max(hits(g, b).astype(jnp.float32), axis=1, keepdims=True)
                bias[g, b] = jnp.broadcast_to(jnp.where(found > 0.0, 0.0, -1e30), (NSEL * SBLK, T))
            return carry

        lax.fori_loop(0, G, one, 0)
        to_smem.wait()

    masks()
    local[0].wait()
    for i in range(Y):
        arrived(ck_slot((y + Y - i) % Y, 1 - k), cdr.at[i])
    local[1].wait()

    def first(c, carry):
        dots(0, s_even, c)
        return carry

    lax.fori_loop(0, NB, first, 0)

    def tick(i, carry):
        ring(i)
        lax.fori_loop(jnp.minimum(3 * (i - 1), G * NB), jnp.minimum(3 * i, G * NB), block, 0)
        return carry

    lax.fori_loop(1, STEPS, tick, 0)
    for n in (G - 2, G - 1):
        send_importance(n).start()

    half = table.at[pl.ds(0, table.shape[0] // 2)]
    arrived(half, dr)

    def send_picked(n):
        g, dev = peer(n)
        return remote(fres.at[g], frecv.at[me], fs.at[n], fr.at[me], dev)

    def fine(n):
        g, _ = peer(n)
        for b in range(NB):
            rows = [table[ids[g, b, s]].astype(jnp.float32) for s in range(NSEL)]
            cand = jnp.concatenate(rows, axis=0).astype(jnp.bfloat16)
            sc = lax.dot_general(
                cand, qb[g, b], (((1,), (1,)), ((), ())), preferred_element_type=jnp.float32
            )
            sc = sc * factor + bias[g, b]
            top = jnp.max(sc, axis=0, keepdims=True)
            e = jnp.exp2(sc - top)
            e = e * (1.0 / jnp.sum(e, axis=0, keepdims=True))
            val = jnp.sum(e, axis=1, keepdims=True)
            fres[g, b:b + 1, :] = jnp.sum(jnp.where(hits(g, b), val, 0.0), axis=0, keepdims=True)

    def fine_step(n, carry):
        m = G - n

        @pl.when(n > 1)
        def _():
            send_picked(m + 1).start()

        fine(m)
        return carry

    lax.fori_loop(1, G, fine_step, 0)
    fine(0)
    send_picked(1).start()
    frecv[me] = fres[me]
    irecv[me] = res[me]

    for n in range(1, G):
        g, _ = peer(n)
        arrived(irecv.at[g], or_.at[g])
    for b in range(NB):
        for j in range(S // D):
            imp_ref[b, j] = irecv[:, b, j, :]
    lane = lax.broadcasted_iota(jnp.int32, (H, D), 1)
    weights = []
    for b in range(NB):
        owner = lax.shift_right_logical(jnp.concatenate([pkv[me, b:b + 1, :]] * 2, axis=1), 3)
        w = jnp.zeros((H, 2 * PICK), jnp.float32)
        for s in range(NSEL):
            sid = ids[me, b, s]
            part = imp_ref[b, lax.shift_right_logical(sid, 7)]
            one = jnp.sum(jnp.where(lane == (sid & (D - 1)), part, 0.0), axis=1, keepdims=True)
            w = w + jnp.where(owner == s, one, 0.0)
        weights.append(w * (PICK / T))
    for n in range(1, G):
        g, _ = peer(n)
        arrived(frecv.at[g], fr.at[g])
    for b in range(NB):
        both = frecv[:, b, :] * weights[b]
        for h in range(0, H, 2):
            sel_ref[b:b + 1, h * PICK:(h + 2) * PICK] = both[h:h + 1] + both[h + 1:h + 2]

    for c in out:
        c.wait_send()
    for n in range(1, G):
        send_importance(n).wait_send()
        send_picked(n).wait_send()
    arrived(table.at[pl.ds(0, STEPS * SUB)], rs)
    arrived(table.at[pl.ds(0, STEPS * SUB)], ls)
    arrived(half, ds)


def per_device(queries, coarse_keys, fine_keys, super_ids, picks):
    nb, t, width = queries.shape
    ch = coarse_keys.shape[0]
    s = ch * Y * K
    dma = pltpu.SemaphoreType.DMA
    f32, bf16, i32 = jnp.float32, jnp.bfloat16, jnp.int32
    imp, sel = pl.pallas_call(
        kernel,
        out_shape=(
            jax.ShapeDtypeStruct((nb, s // D, H, D), f32),
            jax.ShapeDtypeStruct((nb, H * PICK), f32),
        ),
        in_specs=[pl.BlockSpec(memory_space=pl.ANY)] * 5,
        out_specs=[pl.BlockSpec(memory_space=pltpu.VMEM)] * 2,
        scratch_shapes=[
            pltpu.VMEM((s, SBLK, D), bf16),
            pltpu.VMEM((Y * K, ch, D), bf16),
            pltpu.VMEM((G, nb, t, D), bf16),
            pltpu.VMEM((s // D, nb * t, D), f32),
            pltpu.VMEM((s // D, nb * t, D), f32),
            pltpu.VMEM((s // D, t, D), f32),
            pltpu.VMEM((G, nb, NSEL), i32),
            pltpu.VMEM((G, nb, PICK), i32),
            pltpu.SMEM((G, nb, NSEL), i32),
            pltpu.VMEM((G, nb, s // D, D), f32),
            pltpu.VMEM((G, nb, s // D, D), f32),
            pltpu.VMEM((G, nb, 2 * PICK), f32),
            pltpu.VMEM((G, nb, 2 * PICK), f32),
            pltpu.VMEM((G, nb, NSEL * SBLK, t), f32),
            dma((Y - 1,)), dma((Y - 1,)), dma((Y,)), dma((Y,)),
            dma((G - 1,)), dma((G,)), dma((G - 1,)), dma((G,)), dma((G - 1,)), dma((G,)),
            dma((X - 1,)), dma((X - 1,)),
            dma, dma((STEPS,)), dma, dma((STEPS,)), dma, dma,
            dma((G,)), dma((G,)), dma((G,)), dma((G,)), dma((6,)),
        ],
        compiler_params=pltpu.CompilerParams(collective_id=0, has_side_effects=True),
    )(queries, coarse_keys, fine_keys.reshape(-1, SBLK, width), super_ids, picks)
    return imp.transpose(0, 2, 1, 3).reshape(nb, H, s), sel


def solution(mesh):
    return jax.shard_map(
        per_device,
        mesh=mesh,
        in_specs=(
            P(("row", "col"), None, None),
            P("row", None),
            P("col", None),
            P(("row", "col"), None),
            P(("row", "col"), None),
        ),
        out_specs=(P(("row", "col"), None, None), P(("row", "col"), None)),
        check_vma=False,
    )
```

```python
import functools
import math

import jax
import jax.numpy as jnp
from jax import lax
from jax.experimental import pallas as pl
from jax.experimental.pallas import tpu as pltpu
from jax.sharding import PartitionSpec as P

H = 8
D = 128
SBLK = 8
PICK = 64
NSEL = 16
LOG2E = 1.4426950408889634

K, X, Y, Z = 2, 4, 4, 8
G = 2 * Y
SUB = 32
STEPS = 14


def kernel(
    q_ref, ck_ref, fk_ref, pk_ref,
    imp_out, sel_ref,
    table, ck, qb, s_even, s_odd, e_buf, pkv, ids, res, irecv, fres, frecv, bias, imp_ref,
    cs, cr, cds, cdr, qs, qr, ms, mr, xs, xr,
    rs, rr, ls, lr, ds, dr, os_, or_, fs, fr, loc,
):
    NB, T, _ = q_ref.shape
    S = Y * K * ck_ref.shape[0]
    CH = ck_ref.shape[0]
    PER = Y * K // NB
    factor = LOG2E / math.sqrt(D)
    row = lax.axis_index("row")
    col = lax.axis_index("col")
    y, k = row // K, row % K
    z, x = col // X, col % X
    par = x % 2
    me = 2 * y + par

    def at(yy, kk, zz, xx):
        return {"row": yy * K + kk, "col": zz * X + xx}

    def remote(src, dst, send, recv, dev):
        return pltpu.make_async_remote_copy(
            src_ref=src, dst_ref=dst, send_sem=send, recv_sem=recv,
            device_id=dev, device_id_type=pl.DeviceIdType.MESH,
        )

    def arrived(dst, sem):
        pltpu.make_async_copy(dst, dst, sem).wait()

    def peer(n):
        m = n // 2
        yy = (y + m + (m // 2) * (1 - 2 * (m % 2))) % Y
        pp = (par + n) % 2
        return 2 * yy + pp, at(yy, k, z, (x // 2) * 2 + pp)

    def heads(h):
        return pl.ds(pl.multiple_of(h * D, D), D)

    def piece(zz, xx, kk):
        return table.at[pl.ds((zz * X + xx) * (K * SUB) + kk * SUB, SUB)]

    def ck_slot(yy, kk):
        return ck.at[yy * K + kk]

    partner = at(y, 1 - k, z, x)
    right, left = at(y, k, (z + 1) % Z, x), at(y, k, (z + Z - 1) % Z, x)

    greet = [peer(n)[1] for n in range(1, G)]
    greet += [at(y, k, z, (x + 2) % X), at(y, k, z, (x + X - 1 + 2 * par) % X)]
    greet += [right, left, partner]
    barrier = pltpu.get_barrier_semaphore()
    for dev in greet:
        pl.semaphore_signal(barrier, inc=1, device_id=dev, device_id_type=pl.DeviceIdType.MESH)
    pl.semaphore_wait(barrier, len(greet))

    out = []
    for i in range(1, Y):
        yy = (y + i) % Y
        c = remote(ck_ref.at[:, heads(2 * yy + par)], ck_slot(y, k), cs.at[i - 1], cr.at[i - 1],
                   at(yy, k, z, x))
        c.start()
        out.append(c)
    own = fk_ref.at[pl.ds(k * SUB, SUB), :, heads(me)]
    mine = piece(z, x, k)
    remote(own, mine, rs, rr.at[0], right).start()
    remote(own, mine, ls, lr.at[0], left).start()
    for i in range(1, X):
        xx = (x + X - i) % X
        c = remote(fk_ref.at[pl.ds(k * SUB, SUB), :, heads(2 * y + xx % 2)], mine,
                   xs.at[i - 1], xr.at[i - 1], at(y, k, z, xx))
        c.start()
        out.append(c)
    c = remote(ck_ref.at[:, heads(me)], ck_slot(y, k), cds.at[0], cdr.at[0], partner)
    c.start()
    out.append(c)
    remote(own, mine, ds, dr, partner).start()
    local = [
        pltpu.make_async_copy(ck_ref.at[:, heads(me)], ck_slot(y, k), loc.at[0]),
        pltpu.make_async_copy(q_ref.at[:, :, heads(me)], qb.at[me], loc.at[1]),
        pltpu.make_async_copy(own, mine, loc.at[2]),
        pltpu.make_async_copy(pk_ref, pkv.at[me], loc.at[4]),
    ]
    for c in local:
        c.start()
    for n in range(1, G):
        g, dev = peer(n)
        c = remote(pk_ref, pkv.at[me], ms.at[n - 1], mr.at[me], dev)
        c.start()
        out.append(c)
    for n in range(1, G):
        g, dev = peer(n)
        c = remote(q_ref.at[:, :, heads(g)], qb.at[me], qs.at[n - 1], qr.at[me], dev)
        c.start()
        out.append(c)

    for s in range(1, X):
        p = piece(z, (x + s) % X, k)
        arrived(p, xr.at[s - 1])
        remote(p, p, rs, rr.at[s], right).start()
        remote(p, p, ls, lr.at[s], left).start()
        remote(p, p, ds, dr, partner).start()

    def ring(i):
        d = i // X + 1
        sub = i % X
        p = piece((z + Z - d) % Z, (x + sub) % X, k)
        arrived(p, rr.at[i])

        @pl.when(i < STEPS - X)
        def _():
            remote(p, p, rs, rr.at[i + X], right).start()

        remote(p, p, ds, dr, partner).start()
        o = piece((z + d) % Z, (x + sub + 2 * (i // (3 * X))) % X, k)
        arrived(o, lr.at[i])

        @pl.when(i < 2 * X)
        def _():
            remote(o, o, ls, lr.at[i + X], left).start()

        @pl.when((i >= STEPS - X) & (i < 3 * X))
        def _():
            remote(o, o, ls, lr.at[i + 2], left).start()

        remote(o, o, ds, dr, partner).start()

    def wait_queries(n):
        g, _ = peer(n)
        arrived(qb.at[g], qr.at[g])

    def dots(n, s_buf, c):
        g, _ = peer(n)
        qq = qb[g].reshape(NB * T, D)
        for r in range(PER):
            sc = lax.dot_general(
                qq, ck[c * PER + r], (((1,), (1,)), ((), ())), preferred_element_type=jnp.float32
            )
            for j in range(CH // D):
                s_buf[(c * PER + r) * (CH // D) + j] = sc[:, j * D:(j + 1) * D]

    def soften(n, s_buf, b):
        g, _ = peer(n)
        rows = pl.ds(pl.multiple_of(b * T, T), T)
        top = s_buf[0, rows, :]
        for j in range(1, S // D):
            top = jnp.maximum(top, s_buf[j, rows, :])
        top = jnp.max(top, axis=1, keepdims=True) * factor
        z = None
        for j in range(S // D):
            e = jnp.exp2(s_buf[j, rows, :] * factor - top)
            e_buf[j] = e
            z = e if z is None else z + e
        w = (S / T) / jnp.sum(z, axis=1, keepdims=True)
        for j in range(S // D):
            res[g, b, j:j + 1, :] = jnp.sum(e_buf[j] * w, axis=0, keepdims=True)

    def send_importance(n):
        g, dev = peer(n)
        return remote(res.at[g], irecv.at[me], os_.at[n], or_.at[me], dev)

    def block(u, carry):
        n, b = u // NB, u % NB
        nxt = jnp.minimum(n + 1, G - 1)

        @pl.when((b == 0) & (n < G - 1))
        def _():
            wait_queries(nxt)

        @pl.when((b == 0) & (n >= 3))
        def _():
            send_importance(n - 2).start()

        @pl.when(n % 2 == 0)
        def _():
            dots(nxt, s_odd, b)
            soften(n, s_even, b)

        @pl.when(n % 2 == 1)
        def _():
            dots(nxt, s_even, b)
            soften(n, s_odd, b)

        return carry

    ring(0)
    for i in range(1, Y):
        slot = ck_slot((y + Y - i) % Y, k)
        arrived(slot, cr.at[i - 1])
        c = remote(slot, slot, cds.at[i], cdr.at[i], partner)
        c.start()
        out.append(c)
    place = lax.broadcasted_iota(jnp.int32, (NSEL * SBLK, 2 * PICK), 0)
    mine_half = lax.broadcasted_iota(jnp.int32, (1, 2 * PICK), 1) // PICK == par

    def hits(g, b):
        row = jnp.concatenate([pkv[g, b:b + 1, :PICK]] * 2, axis=1)
        return place == jnp.where(mine_half, row, -1)

    def masks():
        for n in range(1, G):
            g, _ = peer(n)
            arrived(pkv.at[g], mr.at[g])
        for c in local[2:]:
            c.wait()
        to_smem = pltpu.make_async_copy(pkv, ids, loc.at[5])
        to_smem.start()

        def one(g, carry):
            for b in range(NB):
                found = jnp.max(hits(g, b).astype(jnp.float32), axis=1, keepdims=True)
                bias[g, b] = jnp.broadcast_to(jnp.where(found > 0.0, 0.0, -1e30), (NSEL * SBLK, T))
            return carry

        lax.fori_loop(0, G, one, 0)
        to_smem.wait()

    masks()
    local[0].wait()
    for i in range(Y):
        arrived(ck_slot((y + Y - i) % Y, 1 - k), cdr.at[i])
    local[1].wait()

    def first(c, carry):
        dots(0, s_even, c)
        return carry

    lax.fori_loop(0, NB, first, 0)

    def tick(i, carry):
        ring(i)
        lax.fori_loop(jnp.minimum(3 * (i - 1), G * NB), jnp.minimum(3 * i, G * NB), block, 0)
        return carry

    lax.fori_loop(1, STEPS, tick, 0)
    for n in (G - 2, G - 1):
        send_importance(n).start()

    half = table.at[pl.ds(0, table.shape[0] // 2)]
    arrived(half, dr)

    def send_picked(n):
        g, dev = peer(n)
        return remote(fres.at[g], frecv.at[me], fs.at[n], fr.at[me], dev)

    def fine(n):
        g, _ = peer(n)
        for b in range(NB):
            rows = [table[ids[g, b, PICK + s]].astype(jnp.float32) for s in range(NSEL)]
            cand = jnp.concatenate(rows, axis=0).astype(jnp.bfloat16)
            sc = lax.dot_general(
                cand, qb[g, b], (((1,), (1,)), ((), ())), preferred_element_type=jnp.float32
            )
            sc = sc * factor + bias[g, b]
            top = jnp.max(sc, axis=0, keepdims=True)
            e = jnp.exp2(sc - top)
            e = e * (1.0 / jnp.sum(e, axis=0, keepdims=True))
            val = jnp.sum(e, axis=1, keepdims=True)
            fres[g, b:b + 1, :] = jnp.sum(jnp.where(hits(g, b), val, 0.0), axis=0, keepdims=True)

    def fine_step(n, carry):
        m = G - n

        @pl.when(n > 1)
        def _():
            send_picked(m + 1).start()

        fine(m)
        return carry

    lax.fori_loop(1, G, fine_step, 0)
    fine(0)
    send_picked(1).start()
    frecv[me] = fres[me]
    irecv[me] = res[me]

    for n in range(1, G):
        g, _ = peer(n)
        arrived(irecv.at[g], or_.at[g])
    for b in range(NB):
        for j in range(S // D):
            imp_ref[b, j] = irecv[:, b, j, :]
    imp_copy = pltpu.make_async_copy(imp_ref, imp_out, loc.at[6])
    imp_copy.start()
    lane = lax.broadcasted_iota(jnp.int32, (H, D), 1)
    weights = []
    for b in range(NB):
        owner = lax.shift_right_logical(jnp.concatenate([pkv[me, b:b + 1, :PICK]] * 2, axis=1), 3)
        w = jnp.zeros((H, 2 * PICK), jnp.float32)
        for s in range(NSEL):
            sid = ids[me, b, PICK + s]
            part = imp_ref[b, lax.shift_right_logical(sid, 7)]
            one = jnp.sum(jnp.where(lane == (sid & (D - 1)), part, 0.0), axis=1, keepdims=True)
            w = w + jnp.where(owner == s, one, 0.0)
        weights.append(w * (PICK / T))
    for n in range(1, G):
        g, _ = peer(n)
        arrived(frecv.at[g], fr.at[g])
    for b in range(NB):
        both = frecv[:, b, :] * weights[b]
        for h in range(0, H, 2):
            sel_ref[b:b + 1, h * PICK:(h + 2) * PICK] = both[h:h + 1] + both[h + 1:h + 2]

    imp_copy.wait()
    for c in out:
        c.wait_send()
    for n in range(1, G):
        send_importance(n).wait_send()
        send_picked(n).wait_send()
    arrived(table.at[pl.ds(0, STEPS * SUB)], rs)
    arrived(table.at[pl.ds(0, STEPS * SUB)], ls)
    arrived(half, ds)


def per_device(queries, coarse_keys, fine_keys, super_ids, picks):
    nb, t, width = queries.shape
    ch = coarse_keys.shape[0]
    s = ch * Y * K
    dma = pltpu.SemaphoreType.DMA
    f32, bf16, i32 = jnp.float32, jnp.bfloat16, jnp.int32
    named = jnp.concatenate([picks, super_ids], axis=1)
    imp, sel = pl.pallas_call(
        kernel,
        out_shape=(
            jax.ShapeDtypeStruct((nb, s // D, H, D), f32),
            jax.ShapeDtypeStruct((nb, H * PICK), f32),
        ),
        in_specs=[pl.BlockSpec(memory_space=pl.ANY)] * 4,
        out_specs=[pl.BlockSpec(memory_space=pl.ANY), pl.BlockSpec(memory_space=pltpu.VMEM)],
        scratch_shapes=[
            pltpu.VMEM((s, SBLK, D), bf16),
            pltpu.VMEM((Y * K, ch, D), bf16),
            pltpu.VMEM((G, nb, t, D), bf16),
            pltpu.VMEM((s // D, nb * t, D), f32),
            pltpu.VMEM((s // D, nb * t, D), f32),
            pltpu.VMEM((s // D, t, D), f32),
            pltpu.VMEM((G, nb, PICK + NSEL), i32),
            pltpu.SMEM((G, nb, PICK + NSEL), i32),
            pltpu.VMEM((G, nb, s // D, D), f32),
            pltpu.VMEM((G, nb, s // D, D), f32),
            pltpu.VMEM((G, nb, 2 * PICK), f32),
            pltpu.VMEM((G, nb, 2 * PICK), f32),
            pltpu.VMEM((G, nb, NSEL * SBLK, t), f32),
            pltpu.VMEM((nb, s // D, H, D), f32),
            dma((Y - 1,)), dma((Y - 1,)), dma((Y,)), dma((Y,)),
            dma((G - 1,)), dma((G,)), dma((G - 1,)), dma((G,)),
            dma((X - 1,)), dma((X - 1,)),
            dma, dma((STEPS,)), dma, dma((STEPS,)), dma, dma,
            dma((G,)), dma((G,)), dma((G,)), dma((G,)), dma((7,)),
        ],
        compiler_params=pltpu.CompilerParams(collective_id=0, has_side_effects=True, vmem_limit_bytes=56_000_000),
    )(queries, coarse_keys, fine_keys.reshape(-1, SBLK, width), named)
    return imp.transpose(0, 2, 1, 3).reshape(nb, H, s), sel


def solution(mesh):
    return jax.shard_map(
        per_device,
        mesh=mesh,
        in_specs=(
            P(("row", "col"), None, None),
            P("row", None),
            P("col", None),
            P(("row", "col"), None),
            P(("row", "col"), None),
        ),
        out_specs=(P(("row", "col"), None, None), P(("row", "col"), None)),
        check_vma=False,
    )
```

```python
import functools
import math

import jax
import jax.numpy as jnp
from jax import lax
from jax.experimental import pallas as pl
from jax.experimental.pallas import tpu as pltpu
from jax.sharding import PartitionSpec as P

H = 8
D = 128
SBLK = 8
PICK = 64
NSEL = 16
LOG2E = 1.4426950408889634

K, X, Y, Z = 2, 4, 4, 8
G = 2 * Y
SUB = 32
STEPS = 14


def kernel(
    q_ref, ck_ref, fk_ref, pk_ref,
    imp_out, sel_ref,
    table, ck, qb, s_even, s_odd, e_buf, pkv, ids, res, irecv, fres, frecv, bias, imp_ref,
    cs, cr, cds, cdr, qs, qr, ms, mr, xs, xr,
    rs, rr, ls, lr, ds, dr, os_, or_, fs, fr, loc,
):
    NB, T, _ = q_ref.shape
    S = Y * K * ck_ref.shape[0]
    CH = ck_ref.shape[0]
    PER = Y * K // NB
    factor = LOG2E / math.sqrt(D)
    row = lax.axis_index("row")
    col = lax.axis_index("col")
    y, k = row // K, row % K
    z, x = col // X, col % X
    par = x % 2
    me = 2 * y + par

    def at(yy, kk, zz, xx):
        return {"row": yy * K + kk, "col": zz * X + xx}

    def remote(src, dst, send, recv, dev):
        return pltpu.make_async_remote_copy(
            src_ref=src, dst_ref=dst, send_sem=send, recv_sem=recv,
            device_id=dev, device_id_type=pl.DeviceIdType.MESH,
        )

    def arrived(dst, sem):
        pltpu.make_async_copy(dst, dst, sem).wait()

    def peer(n):
        m = n // 2
        yy = (y + m + (m // 2) * (1 - 2 * (m % 2))) % Y
        pp = (par + n) % 2
        return 2 * yy + pp, at(yy, k, z, (x // 2) * 2 + pp)

    def heads(h):
        return pl.ds(pl.multiple_of(h * D, D), D)

    def piece(zz, xx, kk):
        return table.at[pl.ds((zz * X + xx) * (K * SUB) + kk * SUB, SUB)]

    def ck_slot(yy, kk):
        return ck.at[yy * K + kk]

    partner = at(y, 1 - k, z, x)
    right, left = at(y, k, (z + 1) % Z, x), at(y, k, (z + Z - 1) % Z, x)

    greet = [peer(n)[1] for n in range(1, G)]
    greet += [at(y, k, z, (x + 2) % X), at(y, k, z, (x + X - 1 + 2 * par) % X)]
    greet += [right, left, partner]
    barrier = pltpu.get_barrier_semaphore()
    for dev in greet:
        pl.semaphore_signal(barrier, inc=1, device_id=dev, device_id_type=pl.DeviceIdType.MESH)
    pl.semaphore_wait(barrier, len(greet))

    out = []
    for i in range(1, Y):
        yy = (y + i) % Y
        c = remote(ck_ref.at[:, heads(2 * yy + par)], ck_slot(y, k), cs.at[i - 1], cr.at[i - 1],
                   at(yy, k, z, x))
        c.start()
        out.append(c)
    own = fk_ref.at[pl.ds(k * SUB, SUB), :, heads(me)]
    mine = piece(z, x, k)
    remote(own, mine, rs, rr.at[0], right).start()
    remote(own, mine, ls, lr.at[0], left).start()
    for i in range(1, X):
        xx = (x + X - i) % X
        c = remote(fk_ref.at[pl.ds(k * SUB, SUB), :, heads(2 * y + xx % 2)], mine,
                   xs.at[i - 1], xr.at[i - 1], at(y, k, z, xx))
        c.start()
        out.append(c)
    c = remote(ck_ref.at[:, heads(me)], ck_slot(y, k), cds.at[0], cdr.at[0], partner)
    c.start()
    out.append(c)
    remote(own, mine, ds, dr, partner).start()
    local = [
        pltpu.make_async_copy(ck_ref.at[:, heads(me)], ck_slot(y, k), loc.at[0]),
        pltpu.make_async_copy(q_ref.at[:, :, heads(me)], qb.at[me], loc.at[1]),
        pltpu.make_async_copy(own, mine, loc.at[2]),
        pltpu.make_async_copy(pk_ref, pkv.at[me], loc.at[4]),
    ]
    for c in local:
        c.start()
    for n in range(1, G):
        g, dev = peer(n)
        c = remote(pk_ref, pkv.at[me], ms.at[n - 1], mr.at[me], dev)
        c.start()
        out.append(c)
    for n in range(1, G):
        g, dev = peer(n)
        c = remote(q_ref.at[:, :, heads(g)], qb.at[me], qs.at[n - 1], qr.at[me], dev)
        c.start()
        out.append(c)

    for s in range(1, X):
        p = piece(z, (x + s) % X, k)
        arrived(p, xr.at[s - 1])
        remote(p, p, rs, rr.at[s], right).start()
        remote(p, p, ls, lr.at[s], left).start()
        remote(p, p, ds, dr, partner).start()

    def ring(i):
        d = i // X + 1
        sub = i % X
        p = piece((z + Z - d) % Z, (x + sub) % X, k)
        arrived(p, rr.at[i])

        @pl.when(i < STEPS - X)
        def _():
            remote(p, p, rs, rr.at[i + X], right).start()

        remote(p, p, ds, dr, partner).start()
        o = piece((z + d) % Z, (x + sub + 2 * (i // (3 * X))) % X, k)
        arrived(o, lr.at[i])

        @pl.when(i < 2 * X)
        def _():
            remote(o, o, ls, lr.at[i + X], left).start()

        @pl.when((i >= STEPS - X) & (i < 3 * X))
        def _():
            remote(o, o, ls, lr.at[i + 2], left).start()

        remote(o, o, ds, dr, partner).start()

    def wait_queries(n):
        g, _ = peer(n)
        arrived(qb.at[g], qr.at[g])

    def dots(n, s_buf, c):
        g, _ = peer(n)
        qq = qb[g].reshape(NB * T, D)
        for r in range(PER):
            sc = lax.dot_general(
                qq, ck[c * PER + r], (((1,), (1,)), ((), ())), preferred_element_type=jnp.float32
            )
            for j in range(CH // D):
                s_buf[(c * PER + r) * (CH // D) + j] = sc[:, j * D:(j + 1) * D]

    def soften(n, s_buf, b):
        g, _ = peer(n)
        rows = pl.ds(pl.multiple_of(b * T, T), T)
        top = s_buf[0, rows, :]
        for j in range(1, S // D):
            top = jnp.maximum(top, s_buf[j, rows, :])
        top = jnp.max(top, axis=1, keepdims=True) * factor
        z = None
        for j in range(S // D):
            e = jnp.exp2(s_buf[j, rows, :] * factor - top)
            e_buf[j] = e
            z = e if z is None else z + e
        w = (S / T) / jnp.sum(z, axis=1, keepdims=True)
        for j in range(S // D):
            res[g, b, j:j + 1, :] = jnp.sum(e_buf[j] * w, axis=0, keepdims=True)

    def send_importance(n):
        g, dev = peer(n)
        return remote(res.at[g], irecv.at[me], os_.at[n], or_.at[me], dev)

    def block(u, carry):
        n, b = u // NB, u % NB
        nxt = jnp.minimum(n + 1, G - 1)

        @pl.when((b == 0) & (n < G - 1))
        def _():
            wait_queries(nxt)

        @pl.when((b == 0) & (n >= 3))
        def _():
            send_importance(n - 2).start()

        @pl.when(n % 2 == 0)
        def _():
            dots(nxt, s_odd, b)
            soften(n, s_even, b)

        @pl.when(n % 2 == 1)
        def _():
            dots(nxt, s_even, b)
            soften(n, s_odd, b)

        return carry

    ring(0)
    for i in range(1, Y):
        slot = ck_slot((y + Y - i) % Y, k)
        arrived(slot, cr.at[i - 1])
        c = remote(slot, slot, cds.at[i], cdr.at[i], partner)
        c.start()
        out.append(c)
    place = lax.broadcasted_iota(jnp.int32, (NSEL * SBLK, 2 * PICK), 0)
    mine_half = lax.broadcasted_iota(jnp.int32, (1, 2 * PICK), 1) // PICK == par

    def hits(g, b):
        row = jnp.concatenate([pkv[g, b:b + 1, :PICK]] * 2, axis=1)
        return place == jnp.where(mine_half, row, -1)

    def masks():
        for n in range(1, G):
            g, _ = peer(n)
            arrived(pkv.at[g], mr.at[g])
        for c in local[2:]:
            c.wait()
        to_smem = pltpu.make_async_copy(pkv, ids, loc.at[5])
        to_smem.start()

        def one(g, carry):
            for b in range(NB):
                found = jnp.max(hits(g, b).astype(jnp.float32), axis=1, keepdims=True)
                bias[g, b] = jnp.broadcast_to(jnp.where(found > 0.0, 0.0, -1e30), (NSEL * SBLK, T))
            return carry

        lax.fori_loop(0, G, one, 0)
        to_smem.wait()

    masks()
    local[0].wait()
    for i in range(Y):
        arrived(ck_slot((y + Y - i) % Y, 1 - k), cdr.at[i])
    local[1].wait()

    def first(c, carry):
        dots(0, s_even, c)
        return carry

    lax.fori_loop(0, NB, first, 0)

    def tick(i, carry):
        ring(i)
        lax.fori_loop(jnp.minimum(3 * (i - 1), G * NB), jnp.minimum(3 * i, G * NB), block, 0)
        return carry

    lax.fori_loop(1, STEPS, tick, 0)
    for n in (G - 2, G - 1):
        send_importance(n).start()

    half = table.at[pl.ds(0, table.shape[0] // 2)]
    arrived(half, dr)

    def send_picked(n):
        g, dev = peer(n)
        return remote(fres.at[g], frecv.at[me], fs.at[n], fr.at[me], dev)

    def fine(n):
        g, _ = peer(n)
        for b in range(NB):
            rows = [table[ids[g, b, PICK + s]].astype(jnp.float32) for s in range(NSEL)]
            cand = jnp.concatenate(rows, axis=0).astype(jnp.bfloat16)
            sc = lax.dot_general(
                cand, qb[g, b], (((1,), (1,)), ((), ())), preferred_element_type=jnp.float32
            )
            sc = sc * factor + bias[g, b]
            top = jnp.max(sc, axis=0, keepdims=True)
            e = jnp.exp2(sc - top)
            e = e * (1.0 / jnp.sum(e, axis=0, keepdims=True))
            val = jnp.sum(e, axis=1, keepdims=True)
            fres[g, b:b + 1, :] = jnp.sum(jnp.where(hits(g, b), val, 0.0), axis=0, keepdims=True)

    def fine_step(n, carry):
        m = G - 1 - 2 * n

        @pl.when(n > 0)
        def _():
            send_picked(m + 2).start()
            send_picked(m + 1).start()

        fine(m)
        fine(m - 1)
        return carry

    lax.fori_loop(0, G // 2, fine_step, 0)
    send_picked(1).start()
    frecv[me] = fres[me]
    irecv[me] = res[me]

    for n in range(1, G):
        g, _ = peer(n)
        arrived(irecv.at[g], or_.at[g])
    for b in range(NB):
        for j in range(S // D):
            imp_ref[b, j] = irecv[:, b, j, :]
    imp_copy = pltpu.make_async_copy(imp_ref, imp_out, loc.at[6])
    imp_copy.start()
    lane = lax.broadcasted_iota(jnp.int32, (H, D), 1)
    weights = []
    for b in range(NB):
        owner = lax.shift_right_logical(jnp.concatenate([pkv[me, b:b + 1, :PICK]] * 2, axis=1), 3)
        w = jnp.zeros((H, 2 * PICK), jnp.float32)
        for s in range(NSEL):
            sid = ids[me, b, PICK + s]
            part = imp_ref[b, lax.shift_right_logical(sid, 7)]
            one = jnp.sum(jnp.where(lane == (sid & (D - 1)), part, 0.0), axis=1, keepdims=True)
            w = w + jnp.where(owner == s, one, 0.0)
        weights.append(w * (PICK / T))
    for n in range(1, G):
        g, _ = peer(n)
        arrived(frecv.at[g], fr.at[g])
    for b in range(NB):
        both = frecv[:, b, :] * weights[b]
        for h in range(0, H, 2):
            sel_ref[b:b + 1, h * PICK:(h + 2) * PICK] = both[h:h + 1] + both[h + 1:h + 2]

    imp_copy.wait()
    for c in out:
        c.wait_send()
    for n in range(1, G):
        send_importance(n).wait_send()
        send_picked(n).wait_send()
    arrived(table.at[pl.ds(0, STEPS * SUB)], rs)
    arrived(table.at[pl.ds(0, STEPS * SUB)], ls)
    arrived(half, ds)


def per_device(queries, coarse_keys, fine_keys, super_ids, picks):
    nb, t, width = queries.shape
    ch = coarse_keys.shape[0]
    s = ch * Y * K
    dma = pltpu.SemaphoreType.DMA
    f32, bf16, i32 = jnp.float32, jnp.bfloat16, jnp.int32
    named = jnp.concatenate([picks, super_ids], axis=1)
    imp, sel = pl.pallas_call(
        kernel,
        out_shape=(
            jax.ShapeDtypeStruct((nb, s // D, H, D), f32),
            jax.ShapeDtypeStruct((nb, H * PICK), f32),
        ),
        in_specs=[pl.BlockSpec(memory_space=pl.ANY)] * 4,
        out_specs=[pl.BlockSpec(memory_space=pl.ANY), pl.BlockSpec(memory_space=pltpu.VMEM)],
        scratch_shapes=[
            pltpu.VMEM((s, SBLK, D), bf16),
            pltpu.VMEM((Y * K, ch, D), bf16),
            pltpu.VMEM((G, nb, t, D), bf16),
            pltpu.VMEM((s // D, nb * t, D), f32),
            pltpu.VMEM((s // D, nb * t, D), f32),
            pltpu.VMEM((s // D, t, D), f32),
            pltpu.VMEM((G, nb, PICK + NSEL), i32),
            pltpu.SMEM((G, nb, PICK + NSEL), i32),
            pltpu.VMEM((G, nb, s // D, D), f32),
            pltpu.VMEM((G, nb, s // D, D), f32),
            pltpu.VMEM((G, nb, 2 * PICK), f32),
            pltpu.VMEM((G, nb, 2 * PICK), f32),
            pltpu.VMEM((G, nb, NSEL * SBLK, t), f32),
            pltpu.VMEM((nb, s // D, H, D), f32),
            dma((Y - 1,)), dma((Y - 1,)), dma((Y,)), dma((Y,)),
            dma((G - 1,)), dma((G,)), dma((G - 1,)), dma((G,)),
            dma((X - 1,)), dma((X - 1,)),
            dma, dma((STEPS,)), dma, dma((STEPS,)), dma, dma,
            dma((G,)), dma((G,)), dma((G,)), dma((G,)), dma((7,)),
        ],
        compiler_params=pltpu.CompilerParams(collective_id=0, has_side_effects=True, vmem_limit_bytes=56_000_000),
    )(queries, coarse_keys, fine_keys.reshape(-1, SBLK, width), named)
    return imp.transpose(0, 2, 1, 3).reshape(nb, H, s), sel


def solution(mesh):
    return jax.shard_map(
        per_device,
        mesh=mesh,
        in_specs=(
            P(("row", "col"), None, None),
            P("row", None),
            P("col", None),
            P(("row", "col"), None),
            P(("row", "col"), None),
        ),
        out_specs=(P(("row", "col"), None, None), P(("row", "col"), None)),
        check_vma=False,
    )
```

```python
import functools
import math

import jax
import jax.numpy as jnp
from jax import lax
from jax.experimental import pallas as pl
from jax.experimental.pallas import tpu as pltpu
from jax.sharding import PartitionSpec as P

H = 8
D = 128
SBLK = 8
PICK = 64
NSEL = 16
LOG2E = 1.4426950408889634

K, X, Y, Z = 2, 4, 4, 8
G = 2 * Y
SUB = 32
STEPS = 14


def kernel(
    q_ref, ck_ref, fk_ref, pk_ref,
    imp_out, sel_ref,
    table, ck, qb, s_even, s_odd, e_buf, pkv, ids, res, irecv, fres, frecv, bias, imp_ref,
    cs, cr, cds, cdr, qs, qr, ms, mr, xs, xr,
    rs, rr, ls, lr, ds, dr, os_, or_, fs, fr, loc,
):
    NB, T, _ = q_ref.shape
    S = Y * K * ck_ref.shape[0]
    CH = ck_ref.shape[0]
    PER = Y * K // NB
    factor = LOG2E / math.sqrt(D)
    row = lax.axis_index("row")
    col = lax.axis_index("col")
    y, k = row // K, row % K
    z, x = col // X, col % X
    par = x % 2
    me = 2 * y + par

    def at(yy, kk, zz, xx):
        return {"row": yy * K + kk, "col": zz * X + xx}

    def remote(src, dst, send, recv, dev):
        return pltpu.make_async_remote_copy(
            src_ref=src, dst_ref=dst, send_sem=send, recv_sem=recv,
            device_id=dev, device_id_type=pl.DeviceIdType.MESH,
        )

    def arrived(dst, sem):
        pltpu.make_async_copy(dst, dst, sem).wait()

    def peer(n):
        m = n // 2
        yy = (y + m + (m // 2) * (1 - 2 * (m % 2))) % Y
        pp = (par + n) % 2
        return 2 * yy + pp, at(yy, k, z, (x // 2) * 2 + pp)

    def heads(h):
        return pl.ds(pl.multiple_of(h * D, D), D)

    def piece(zz, xx, kk):
        return table.at[pl.ds((zz * X + xx) * (K * SUB) + kk * SUB, SUB)]

    def ck_slot(yy, kk):
        return ck.at[yy * K + kk]

    partner = at(y, 1 - k, z, x)
    right, left = at(y, k, (z + 1) % Z, x), at(y, k, (z + Z - 1) % Z, x)

    greet = [peer(n)[1] for n in range(1, G)]
    greet += [at(y, k, z, (x + 2) % X), at(y, k, z, (x + X - 1 + 2 * par) % X)]
    greet += [right, left, partner]
    barrier = pltpu.get_barrier_semaphore()
    for dev in greet:
        pl.semaphore_signal(barrier, inc=1, device_id=dev, device_id_type=pl.DeviceIdType.MESH)
    pl.semaphore_wait(barrier, len(greet))

    out = []
    for i in range(1, Y):
        yy = (y + i) % Y
        c = remote(ck_ref.at[:, heads(2 * yy + par)], ck_slot(y, k), cs.at[i - 1], cr.at[i - 1],
                   at(yy, k, z, x))
        c.start()
        out.append(c)
    own = fk_ref.at[pl.ds(k * SUB, SUB), :, heads(me)]
    mine = piece(z, x, k)
    remote(own, mine, rs, rr.at[0], right).start()
    remote(own, mine, ls, lr.at[0], left).start()
    for i in range(1, X):
        xx = (x + X - i) % X
        c = remote(fk_ref.at[pl.ds(k * SUB, SUB), :, heads(2 * y + xx % 2)], mine,
                   xs.at[i - 1], xr.at[i - 1], at(y, k, z, xx))
        c.start()
        out.append(c)
    c = remote(ck_ref.at[:, heads(me)], ck_slot(y, k), cds.at[0], cdr.at[0], partner)
    c.start()
    out.append(c)
    remote(own, mine, ds, dr, partner).start()
    local = [
        pltpu.make_async_copy(ck_ref.at[:, heads(me)], ck_slot(y, k), loc.at[0]),
        pltpu.make_async_copy(q_ref.at[:, :, heads(me)], qb.at[me], loc.at[1]),
        pltpu.make_async_copy(own, mine, loc.at[2]),
        pltpu.make_async_copy(pk_ref, pkv.at[me], loc.at[4]),
    ]
    for c in local:
        c.start()
    for n in range(1, G):
        g, dev = peer(n)
        c = remote(pk_ref, pkv.at[me], ms.at[n - 1], mr.at[me], dev)
        c.start()
        out.append(c)
    for n in range(1, G):
        g, dev = peer(n)
        c = remote(q_ref.at[:, :, heads(g)], qb.at[me], qs.at[n - 1], qr.at[me], dev)
        c.start()
        out.append(c)

    for s in range(1, X):
        p = piece(z, (x + s) % X, k)
        arrived(p, xr.at[s - 1])
        remote(p, p, rs, rr.at[s], right).start()
        remote(p, p, ls, lr.at[s], left).start()
        remote(p, p, ds, dr, partner).start()

    def ring(i):
        d = i // X + 1
        sub = i % X
        p = piece((z + Z - d) % Z, (x + sub) % X, k)
        arrived(p, rr.at[i])

        @pl.when(i < STEPS - X)
        def _():
            remote(p, p, rs, rr.at[i + X], right).start()

        remote(p, p, ds, dr, partner).start()
        o = piece((z + d) % Z, (x + sub + 2 * (i // (3 * X))) % X, k)
        arrived(o, lr.at[i])

        @pl.when(i < 2 * X)
        def _():
            remote(o, o, ls, lr.at[i + X], left).start()

        @pl.when((i >= STEPS - X) & (i < 3 * X))
        def _():
            remote(o, o, ls, lr.at[i + 2], left).start()

        remote(o, o, ds, dr, partner).start()

    def wait_queries(n):
        g, _ = peer(n)
        arrived(qb.at[g], qr.at[g])

    def dots(n, s_buf, c):
        g, _ = peer(n)
        qq = qb[g].reshape(NB * T, D)
        for r in range(PER):
            sc = lax.dot_general(
                qq, ck[c * PER + r], (((1,), (1,)), ((), ())), preferred_element_type=jnp.float32
            )
            for j in range(CH // D):
                s_buf[(c * PER + r) * (CH // D) + j] = sc[:, j * D:(j + 1) * D]

    def soften(n, s_buf, b):
        g, _ = peer(n)
        rows = pl.ds(pl.multiple_of(b * T, T), T)
        top = s_buf[0, rows, :]
        for j in range(1, S // D):
            top = jnp.maximum(top, s_buf[j, rows, :])
        top = jnp.max(top, axis=1, keepdims=True) * factor
        z = None
        for j in range(S // D):
            e = jnp.exp2(s_buf[j, rows, :] * factor - top)
            e_buf[j] = e
            z = e if z is None else z + e
        w = (S / T) / jnp.sum(z, axis=1, keepdims=True)
        for j in range(S // D):
            res[g, b, j:j + 1, :] = jnp.sum(e_buf[j] * w, axis=0, keepdims=True)

    def send_importance(n):
        g, dev = peer(n)
        return remote(res.at[g], irecv.at[me], os_.at[n], or_.at[me], dev)

    def block(u, carry):
        n, b = u // NB, u % NB
        nxt = jnp.minimum(n + 1, G - 1)

        @pl.when((b == 0) & (n < G - 1))
        def _():
            wait_queries(nxt)

        @pl.when((b == 0) & (n >= 3))
        def _():
            send_importance(n - 2).start()

        @pl.when(n % 2 == 0)
        def _():
            dots(nxt, s_odd, b)
            soften(n, s_even, b)

        @pl.when(n % 2 == 1)
        def _():
            dots(nxt, s_even, b)
            soften(n, s_odd, b)

        return carry

    ring(0)
    for i in range(1, Y):
        slot = ck_slot((y + Y - i) % Y, k)
        arrived(slot, cr.at[i - 1])
        c = remote(slot, slot, cds.at[i], cdr.at[i], partner)
        c.start()
        out.append(c)
    place = lax.broadcasted_iota(jnp.int32, (NSEL * SBLK, 2 * PICK), 0)
    mine_half = lax.broadcasted_iota(jnp.int32, (1, 2 * PICK), 1) // PICK == par

    def hits(g, b):
        row = jnp.concatenate([pkv[g, b:b + 1, :PICK]] * 2, axis=1)
        return place == jnp.where(mine_half, row, -1)

    def masks():
        for n in range(1, G):
            g, _ = peer(n)
            arrived(pkv.at[g], mr.at[g])
        for c in local[2:]:
            c.wait()
        to_smem = pltpu.make_async_copy(pkv, ids, loc.at[5])
        to_smem.start()

        def one(g, carry):
            for b in range(NB):
                found = jnp.max(hits(g, b).astype(jnp.float32), axis=1, keepdims=True)
                bias[g, b] = jnp.broadcast_to(jnp.where(found > 0.0, 0.0, -1e30), (NSEL * SBLK, T))
            return carry

        lax.fori_loop(0, G, one, 0, unroll=2)
        to_smem.wait()

    masks()
    local[0].wait()
    for i in range(Y):
        arrived(ck_slot((y + Y - i) % Y, 1 - k), cdr.at[i])
    local[1].wait()

    def first(c, carry):
        dots(0, s_even, c)
        return carry

    lax.fori_loop(0, NB, first, 0)

    def tick(i, carry):
        ring(i)
        lax.fori_loop(jnp.minimum(3 * (i - 1), G * NB), jnp.minimum(3 * i, G * NB), block, 0)
        return carry

    lax.fori_loop(1, STEPS, tick, 0)
    for n in (G - 2, G - 1):
        send_importance(n).start()

    half = table.at[pl.ds(0, table.shape[0] // 2)]
    arrived(half, dr)

    def send_picked(n):
        g, dev = peer(n)
        return remote(fres.at[g], frecv.at[me], fs.at[n], fr.at[me], dev)

    def fine(n):
        g, _ = peer(n)
        for b in range(NB):
            rows = [table[ids[g, b, PICK + s]].astype(jnp.float32) for s in range(NSEL)]
            cand = jnp.concatenate(rows, axis=0).astype(jnp.bfloat16)
            sc = lax.dot_general(
                cand, qb[g, b], (((1,), (1,)), ((), ())), preferred_element_type=jnp.float32
            )
            sc = sc * factor + bias[g, b]
            top = jnp.max(sc, axis=0, keepdims=True)
            e = jnp.exp2(sc - top)
            e = e * (1.0 / jnp.sum(e, axis=0, keepdims=True))
            val = jnp.sum(e, axis=1, keepdims=True)
            fres[g, b:b + 1, :] = jnp.sum(jnp.where(hits(g, b), val, 0.0), axis=0, keepdims=True)

    def fine_step(n, carry):
        m = G - 1 - 2 * n

        @pl.when(n > 0)
        def _():
            send_picked(m + 2).start()
            send_picked(m + 1).start()

        fine(m)
        fine(m - 1)
        return carry

    lax.fori_loop(0, G // 2, fine_step, 0)
    send_picked(1).start()
    frecv[me] = fres[me]
    irecv[me] = res[me]

    for n in range(1, G):
        g, _ = peer(n)
        arrived(irecv.at[g], or_.at[g])
    for b in range(NB):
        for j in range(S // D):
            imp_ref[b, j] = irecv[:, b, j, :]
    imp_copy = pltpu.make_async_copy(imp_ref, imp_out, loc.at[6])
    imp_copy.start()
    lane = lax.broadcasted_iota(jnp.int32, (H, D), 1)
    weights = []
    for b in range(NB):
        owner = lax.shift_right_logical(jnp.concatenate([pkv[me, b:b + 1, :PICK]] * 2, axis=1), 3)
        w = jnp.zeros((H, 2 * PICK), jnp.float32)
        for s in range(NSEL):
            sid = ids[me, b, PICK + s]
            part = imp_ref[b, lax.shift_right_logical(sid, 7)]
            one = jnp.sum(jnp.where(lane == (sid & (D - 1)), part, 0.0), axis=1, keepdims=True)
            w = w + jnp.where(owner == s, one, 0.0)
        weights.append(w * (PICK / T))
    for n in range(1, G):
        g, _ = peer(n)
        arrived(frecv.at[g], fr.at[g])
    for b in range(NB):
        both = frecv[:, b, :] * weights[b]
        for h in range(0, H, 2):
            sel_ref[b:b + 1, h * PICK:(h + 2) * PICK] = both[h:h + 1] + both[h + 1:h + 2]

    imp_copy.wait()
    for c in out:
        c.wait_send()
    for n in range(1, G):
        send_importance(n).wait_send()
        send_picked(n).wait_send()
    arrived(table.at[pl.ds(0, STEPS * SUB)], rs)
    arrived(table.at[pl.ds(0, STEPS * SUB)], ls)
    arrived(half, ds)


def per_device(queries, coarse_keys, fine_keys, super_ids, picks):
    nb, t, width = queries.shape
    ch = coarse_keys.shape[0]
    s = ch * Y * K
    dma = pltpu.SemaphoreType.DMA
    f32, bf16, i32 = jnp.float32, jnp.bfloat16, jnp.int32
    named = jnp.concatenate([picks, super_ids], axis=1)
    imp, sel = pl.pallas_call(
        kernel,
        out_shape=(
            jax.ShapeDtypeStruct((nb, s // D, H, D), f32),
            jax.ShapeDtypeStruct((nb, H * PICK), f32),
        ),
        in_specs=[pl.BlockSpec(memory_space=pl.ANY)] * 4,
        out_specs=[pl.BlockSpec(memory_space=pl.ANY), pl.BlockSpec(memory_space=pltpu.VMEM)],
        scratch_shapes=[
            pltpu.VMEM((s, SBLK, D), bf16),
            pltpu.VMEM((Y * K, ch, D), bf16),
            pltpu.VMEM((G, nb, t, D), bf16),
            pltpu.VMEM((s // D, nb * t, D), f32),
            pltpu.VMEM((s // D, nb * t, D), f32),
            pltpu.VMEM((s // D, t, D), f32),
            pltpu.VMEM((G, nb, PICK + NSEL), i32),
            pltpu.SMEM((G, nb, PICK + NSEL), i32),
            pltpu.VMEM((G, nb, s // D, D), f32),
            pltpu.VMEM((G, nb, s // D, D), f32),
            pltpu.VMEM((G, nb, 2 * PICK), f32),
            pltpu.VMEM((G, nb, 2 * PICK), f32),
            pltpu.VMEM((G, nb, NSEL * SBLK, t), f32),
            pltpu.VMEM((nb, s // D, H, D), f32),
            dma((Y - 1,)), dma((Y - 1,)), dma((Y,)), dma((Y,)),
            dma((G - 1,)), dma((G,)), dma((G - 1,)), dma((G,)),
            dma((X - 1,)), dma((X - 1,)),
            dma, dma((STEPS,)), dma, dma((STEPS,)), dma, dma,
            dma((G,)), dma((G,)), dma((G,)), dma((G,)), dma((7,)),
        ],
        compiler_params=pltpu.CompilerParams(collective_id=0, has_side_effects=True, vmem_limit_bytes=56_000_000),
    )(queries, coarse_keys, fine_keys.reshape(-1, SBLK, width), named)
    return imp.transpose(0, 2, 1, 3).reshape(nb, H, s), sel


def solution(mesh):
    return jax.shard_map(
        per_device,
        mesh=mesh,
        in_specs=(
            P(("row", "col"), None, None),
            P("row", None),
            P("col", None),
            P(("row", "col"), None),
            P(("row", "col"), None),
        ),
        out_specs=(P(("row", "col"), None, None), P(("row", "col"), None)),
        check_vma=False,
    )
```
